32 devices in a mesh: head: 4 (over z), outer: 2 (over core), inner: 4 (over y, x).
Axes of the slice: x: 2, y: 2, z: 4, core: 2. Of those that a mesh axis runs over, the one named last changes fastest.
Arguments:
- query: bfloat16 [4096, 8192], P(('outer', 'inner', 'head')), may hold values from -100 to 100
- keys: bfloat16 [4096, 1024], P(('outer', 'inner', 'head')), may hold values from -4.5 to 4.5
- values: bfloat16 [4096, 1024], P(('outer', 'inner', 'head')), may hold values from -6 to 6
- lengths: int32 [8], replicated, may hold values from 1 to 1024, 4096 in all
Outputs:
- attended: bfloat16 [4096, 8192], P(('outer', 'inner', 'head'))
The draws below stay inside these ranges and needn't reach their ends.
Inputs may be any that keep to these rules, and one draw needn't show every extreme that they name: `lengths`: they sum to 4096, and the longest is exactly 1024.
All inputs are finite; a program needn't handle non-finite values.
Results may differ from the reference program's by a relative error of at most 0.0038.
Values may be sent and summed in bfloat16 or wider, within the bound.
A program may use at most 64 MiB of HBM per device.

```python
import math
import jax
import jax.numpy as jnp
import numpy as np
from jax import lax

QUERY_HEAD_COUNT = 64
KEY_VALUE_HEADS = 8
HEAD_SIZE = 128
NEARBY_TOKENS = 512
PACKED_TOKENS = 4096
REACH = 2
MAXDOC = 1024
NDOCS = 8


def starting_keys(key):
    sampled = jnp.clip(jax.random.normal(jax.random.fold_in(key, 30), (PACKED_TOKENS, KEY_VALUE_HEADS * HEAD_SIZE), jnp.float32), -4.5, 4.5)
    return sampled


def draw_keys(key, part):
    return starting_keys(key).astype(jnp.bfloat16)


def draw_query(key, part):
    result = jnp.clip(jax.random.normal(jax.random.fold_in(key, 40), (PACKED_TOKENS, QUERY_HEAD_COUNT * HEAD_SIZE), jnp.float32), -4.5, 4.5)
    return result.astype(jnp.bfloat16)


def block_levels(key, shape, shards, low, high):
    factor_of = 1.0
    for axis_at, parts in shards:
        steps = jax.random.uniform(jax.random.fold_in(jax.random.fold_in(key, 6), axis_at), (parts,), jnp.float32, low / len(shards), high / len(shards))
        factor_of = factor_of * jnp.repeat(jnp.exp(steps), shape[axis_at] // parts).reshape((-1,) + (1,) * (len(shape) - 1 - axis_at))
    return factor_of


def split_up(amount, total, limit, skew):
    loads = [(1 << 20) // math.isqrt(rank ** skew) + 1 for rank in range(2, amount + 1)]
    rest, given = total - limit - (amount - 1), [1] * (amount - 1)
    while rest > 0:
        candidates = [i for i in range(amount - 1) if given[i] < limit]
        pool, remaining = sum([loads[i] for i in candidates]), rest
        for i in candidates:
            addition = min(limit - given[i], max(1, remaining * loads[i] // pool), rest)
            given[i] = given[i] + addition
            rest = rest - addition
    return np.array([limit] + given)


def uneven_parts(stream_key, amount, total, most, lean):
    if amount == 2:
        one = jax.random.randint(stream_key, (), max(1, total - most), min(most, total - 1) + 1)
        return jnp.stack([one, total - one])
    sizes = jnp.asarray(split_up(amount, total, most, lean), jnp.int32)
    twos = (amount - 1) // 2
    donor, taker = sizes[1:1 + 2 * twos:2], sizes[2:2 + 2 * twos:2]
    margin = jnp.minimum(donor - 1, most - taker)
    shifted = jax.random.randint(jax.random.fold_in(stream_key, 1), (twos,), 0, 1 << 20) % (margin + 1)
    sizes = sizes.at[1:1 + 2 * twos:2].set(donor - shifted).at[2:2 + 2 * twos:2].set(taker + shifted)
    return sizes[jax.random.permutation(jax.random.fold_in(stream_key, 2), amount)]


def scatter_about(own_key, extent, deviation, reach, pieces=(), kind=jnp.bfloat16):
    level = block_levels(own_key, extent, pieces, -0.22, 0.18) if pieces else 1.0
    drawn = jax.random.normal(own_key, extent, jnp.float32) * deviation * level
    return jnp.minimum(jnp.maximum(drawn, -reach), reach).astype(kind)


def setup_inputs(seed: int = 0) -> dict:
    streams_of = jax.random.split(jax.random.key(seed), 5)
    query = draw_query(jax.random.fold_in(streams_of[4], 71), 0)
    keys = draw_keys(jax.random.fold_in(streams_of[4], 71), 0)
    values = scatter_about(streams_of[2], (PACKED_TOKENS, KEY_VALUE_HEADS * HEAD_SIZE), 1.0, 6.0, ((0, 32),))
    lengths = uneven_parts(streams_of[3], NDOCS, PACKED_TOKENS, MAXDOC, 2).astype(jnp.int32)
    return dict(query=query, keys=keys, values=values, lengths=lengths)


def doc_of(lengths, positions):
    ends = jnp.cumsum(lengths)
    return lax.optimization_barrier(jnp.sum((positions[:, None] >= ends[None, :]).astype(jnp.int32), axis=1))

def reference(query, keys, values, lengths):
    group_width = QUERY_HEAD_COUNT // KEY_VALUE_HEADS
    trailing_length = REACH * NEARBY_TOKENS
    key_length = trailing_length + NEARBY_TOKENS
    score_scale = 1.0 / math.sqrt(HEAD_SIZE)
    positions = lax.iota(jnp.int32, PACKED_TOKENS)
    docs = doc_of(lengths, positions)
    filled_keys = jnp.concatenate([jnp.zeros((trailing_length, KEY_VALUE_HEADS * HEAD_SIZE), jnp.bfloat16), keys], 0)
    filled_values = jnp.concatenate([jnp.zeros((trailing_length, KEY_VALUE_HEADS * HEAD_SIZE), jnp.bfloat16), values], 0)
    padded_docs = jnp.concatenate([jnp.full((trailing_length,), -1, jnp.int32), docs], 0)

    def one_block(block_index):
        start_row = (block_index * NEARBY_TOKENS).astype(jnp.int32)
        query_matrix = lax.dynamic_slice_in_dim(query, start_row, NEARBY_TOKENS, 0).astype(jnp.float32)
        query_matrix = query_matrix.reshape(NEARBY_TOKENS, KEY_VALUE_HEADS, group_width, HEAD_SIZE)
        key_matrix = lax.dynamic_slice_in_dim(filled_keys, start_row, key_length, 0).astype(jnp.float32)
        key_matrix = key_matrix.reshape(key_length, KEY_VALUE_HEADS, HEAD_SIZE)
        value_matrix = lax.dynamic_slice_in_dim(filled_values, start_row, key_length, 0).astype(jnp.float32)
        value_matrix = value_matrix.reshape(key_length, KEY_VALUE_HEADS, HEAD_SIZE)
        query_docs = lax.dynamic_slice_in_dim(docs, start_row, NEARBY_TOKENS, 0)
        key_docs = lax.dynamic_slice_in_dim(padded_docs, start_row, key_length, 0)
        query_pos = start_row + lax.iota(jnp.int32, NEARBY_TOKENS)
        key_pos = start_row - trailing_length + lax.iota(jnp.int32, key_length)
        visible = (query_docs[:, None] == key_docs[None, :]) & (key_pos[None, :] <= query_pos[:, None])

        def one_head(operands):
            query_heads, key_heads, value_heads = operands
            scores = jnp.einsum('qgd,cd->gqc', query_heads, key_heads) * score_scale
            masked = jnp.where(visible[None], scores, -1e+30)
            top = lax.optimization_barrier(jnp.max(masked, axis=2))
            weights = jnp.where(visible[None], jnp.exp(masked - top[..., None]), 0.0)
            total = lax.optimization_barrier(jnp.sum(weights, axis=2))
            rounded = lax.optimization_barrier(weights.astype(jnp.bfloat16)).astype(jnp.float32)
            summed = jnp.einsum('gqc,cd->qgd', rounded, value_heads)
            return summed / jnp.transpose(total, (1, 0))[..., None]
        per_head = lax.map(one_head, (jnp.transpose(query_matrix, (1, 0, 2, 3)), jnp.transpose(key_matrix, (1, 0, 2)), jnp.transpose(value_matrix, (1, 0, 2))))
        return jnp.transpose(per_head, (1, 0, 2, 3)).reshape(NEARBY_TOKENS, QUERY_HEAD_COUNT * HEAD_SIZE).astype(jnp.bfloat16)
    blocks = lax.map(one_block, lax.iota(jnp.int32, PACKED_TOKENS // NEARBY_TOKENS))
    return blocks.reshape(PACKED_TOKENS, QUERY_HEAD_COUNT * HEAD_SIZE)
```

```python
import functools
import math

import jax
import jax.numpy as jnp
from jax import lax
from jax.experimental import pallas as pl
from jax.experimental.pallas import tpu as pltpu
from jax.sharding import PartitionSpec as P

HEAD_SIZE = 128
MESH = pl.DeviceIdType.MESH


def kernel(
    heads, outers, inners, lengths_ref, q_ref, k_ref, v_ref, out_ref,
    kv, bias, own_sem, z_send, z_recv, y_send, y_recv, x_send, x_recv,
):
    tokens = q_ref.shape[0]
    groups = k_ref.shape[1] // HEAD_SIZE
    width = q_ref.shape[1] // k_ref.shape[1]
    block = heads * tokens
    contexts = outers * inners
    span = (2 * heads + 1) * tokens
    me = lax.axis_index("head")
    ctx = lax.axis_index("outer") * inners + lax.axis_index("inner")
    odd = lax.rem(ctx, 2)

    def context(steps):
        at = lax.rem(ctx + steps + contexts, contexts)
        return {"outer": at // inners, "inner": lax.rem(at, inners)}

    partner = context(1 - 2 * odd)

    def own_copy(g, which):
        ref = (k_ref, v_ref)[which]
        return pltpu.make_async_copy(
            ref.at[:, pl.ds(pl.multiple_of(g * HEAD_SIZE, HEAD_SIZE), HEAD_SIZE)],
            kv.at[g, which, pl.ds(pl.multiple_of(2 * block + me * tokens, tokens), tokens), :],
            own_sem.at[which, g],
        )

    def z_copy(g, distance):
        rows = pl.ds(pl.multiple_of(2 * block + me * tokens, tokens), tokens)
        return pltpu.make_async_remote_copy(
            src_ref=kv.at[g, :, rows, :],
            dst_ref=kv.at[g, :, rows, :],
            send_sem=z_send.at[distance, g],
            recv_sem=z_recv.at[distance, g],
            device_id={"head": lax.rem(me + distance, heads)},
            device_id_type=MESH,
        )

    def z_arrival(g, distance):
        source = lax.rem(me - distance + heads, heads)
        rows = pl.ds(pl.multiple_of(2 * block + source * tokens, tokens), tokens)
        return pltpu.make_async_remote_copy(
            src_ref=kv.at[g, :, rows, :],
            dst_ref=kv.at[g, :, rows, :],
            send_sem=z_send.at[distance, g],
            recv_sem=z_recv.at[distance, g],
            device_id={"head": lax.rem(me + distance, heads)},
            device_id_type=MESH,
        )

    def y_copy(g):
        return pltpu.make_async_remote_copy(
            src_ref=kv.at[g, :, pl.ds(2 * block, block), :],
            dst_ref=kv.at[g, :, pl.ds(0, block), :],
            send_sem=y_send.at[g],
            recv_sem=y_recv.at[g],
            device_id=context(2),
            device_id_type=MESH,
        )

    def x_copy(g):
        start = pl.multiple_of((1 - odd) * 2 * block, block)
        return pltpu.make_async_remote_copy(
            src_ref=kv.at[g, :, pl.ds(start, block), :],
            dst_ref=kv.at[g, :, pl.ds(block, block), :],
            send_sem=x_send.at[g],
            recv_sem=x_recv.at[g],
            device_id=partner,
            device_id_type=MESH,
        )

    for g in range(groups):
        own_copy(g, 0).start()
        own_copy(g, 1).start()

    barrier = pltpu.get_barrier_semaphore()
    for distance in range(1, heads):
        pl.semaphore_signal(
            barrier, inc=1, device_id={"head": lax.rem(me + distance, heads)}, device_id_type=MESH
        )
    for place in (context(2), context(-2), partner):
        pl.semaphore_signal(barrier, inc=1, device_id=place, device_id_type=MESH)
    pl.semaphore_wait(barrier, heads - 1 + 3)

    for g in range(groups):
        own_copy(g, 0).wait()
        own_copy(g, 1).wait()
        for distance in range(1, heads):
            z_copy(g, distance).start()

    first = ctx * block + me * tokens
    query_pos = first + lax.broadcasted_iota(jnp.int32, (tokens, span), 0)
    key_pos = first - 2 * block + lax.broadcasted_iota(jnp.int32, (tokens, span), 1)
    row_pos = first + lax.broadcasted_iota(jnp.int32, (tokens, 128), 0)
    begin = jnp.zeros((tokens, 128), jnp.int32)
    end = jnp.int32(0)
    for n in range(lengths_ref.shape[0]):
        end = end + lengths_ref[n]
        begin = jnp.where(row_pos >= end, end, begin)
    visible = (key_pos >= begin[:, :1]) & (key_pos <= query_pos)
    bias[...] = jnp.where(visible, 0.0, -1e30)

    factor = math.log2(math.e) / math.sqrt(HEAD_SIZE)
    pair = 2 if width % 2 == 0 else 1
    reading = pl.ds(pl.multiple_of(me * tokens, tokens), span)

    def compute(g):
        key_part = kv.at[g, 0]
        value_part = kv.at[g, 1]

        def heads_of(j, carry):
            at = (g * width + j * pair) * HEAD_SIZE
            columns = [
                pl.ds(pl.multiple_of(at + p * HEAD_SIZE, HEAD_SIZE), HEAD_SIZE) for p in range(pair)
            ]
            q = jnp.concatenate([q_ref[:, c] for c in columns], axis=0)
            scores = lax.dot_general(
                q, key_part[reading, :], (((1,), (1,)), ((), ())), preferred_element_type=jnp.float32
            )
            scores = scores.reshape(pair, tokens, span) + bias[...][None]
            scores = scores.reshape(pair * tokens, span)
            top = jnp.max(scores, axis=1, keepdims=True)
            weights = jnp.exp2((scores - top) * factor)
            total = jnp.sum(weights, axis=1, keepdims=True)
            summed = jnp.dot(
                weights.astype(jnp.bfloat16), value_part[reading, :],
                preferred_element_type=jnp.float32,
            )
            result = (summed / total).astype(out_ref.dtype)
            for p in range(pair):
                out_ref[:, columns[p]] = result[p * tokens:(p + 1) * tokens]
            return carry

        lax.fori_loop(0, width // pair, heads_of, 0)

    def step(t, carry):
        @pl.when(t < groups)
        def _():
            for distance in range(1, heads):
                z_arrival(t, distance).wait_recv()
            y_copy(t).start()

            @pl.when(odd == 0)
            def _():
                x_copy(t).start()

        @pl.when((t >= 1) & (t < groups + 1))
        def _():
            y_copy(t - 1).wait_recv()

            @pl.when(odd == 1)
            def _():
                x_copy(t - 1).start()

        @pl.when(t >= 2)
        def _():
            x_copy(t - 2).wait_recv()
            compute(t - 2)

        return carry

    lax.fori_loop(0, groups + 2, step, 0)

    def drain(g, carry):
        for distance in range(1, heads):
            z_copy(g, distance).wait_send()
        y_copy(g).wait_send()
        x_copy(g).wait_send()
        return carry

    lax.fori_loop(0, groups, drain, 0)


def solution(mesh):
    heads, outers, inners = (mesh.shape[name] for name in ("head", "outer", "inner"))

    def per_device(query, keys, values, lengths):
        tokens = query.shape[0]
        groups = keys.shape[1] // HEAD_SIZE
        return pl.pallas_call(
            functools.partial(kernel, heads, outers, inners),
            out_shape=jax.ShapeDtypeStruct(query.shape, query.dtype),
            in_specs=[
                pl.BlockSpec(memory_space=pltpu.SMEM),
                pl.BlockSpec(memory_space=pltpu.VMEM),
                pl.BlockSpec(memory_space=pl.ANY),
                pl.BlockSpec(memory_space=pl.ANY),
            ],
            out_specs=pl.BlockSpec(memory_space=pltpu.VMEM),
            scratch_shapes=[
                pltpu.VMEM((groups, 2, 3 * heads * tokens, HEAD_SIZE), jnp.bfloat16),
                pltpu.VMEM((tokens, (2 * heads + 1) * tokens), jnp.float32),
                pltpu.SemaphoreType.DMA((2, groups)),
                pltpu.SemaphoreType.DMA((heads, groups)),
                pltpu.SemaphoreType.DMA((heads, groups)),
                pltpu.SemaphoreType.DMA((groups,)),
                pltpu.SemaphoreType.DMA((groups,)),
                pltpu.SemaphoreType.DMA((groups,)),
                pltpu.SemaphoreType.DMA((groups,)),
            ],
            compiler_params=pltpu.CompilerParams(collective_id=0, has_side_effects=True),
        )(lengths, query, keys, values)

    rows = P(("outer", "inner", "head"), None)
    return jax.shard_map(
        per_device,
        mesh=mesh,
        in_specs=(rows, rows, rows, P()),
        out_specs=rows,
        check_vma=False,
    )
```

```python
import functools
import math

import jax
import jax.numpy as jnp
from jax import lax
from jax.experimental import pallas as pl
from jax.experimental.pallas import tpu as pltpu
from jax.sharding import PartitionSpec as P

HEAD_SIZE = 128
MESH = pl.DeviceIdType.MESH


def kernel(
    heads, outers, inners, lengths_ref, q_ref, k_ref, v_ref, out_ref,
    kv, bias, own_sem, z_send, z_recv, y_send, y_recv, x_send, x_recv,
):
    tokens = q_ref.shape[0]
    groups = k_ref.shape[1] // HEAD_SIZE
    width = q_ref.shape[1] // k_ref.shape[1]
    block = heads * tokens
    contexts = outers * inners
    span = (2 * heads + 1) * tokens
    me = lax.axis_index("head")
    ctx = lax.axis_index("outer") * inners + lax.axis_index("inner")
    odd = lax.rem(ctx, 2)

    def context(steps):
        at = lax.rem(ctx + steps + contexts, contexts)
        return {"outer": at // inners, "inner": lax.rem(at, inners)}

    partner = context(1 - 2 * odd)

    def own_copy(g, which):
        ref = (k_ref, v_ref)[which]
        return pltpu.make_async_copy(
            ref.at[:, pl.ds(pl.multiple_of(g * HEAD_SIZE, HEAD_SIZE), HEAD_SIZE)],
            kv.at[g, which, pl.ds(pl.multiple_of(2 * block + me * tokens, tokens), tokens), :],
            own_sem.at[which, g],
        )

    def z_copy(g, shard, way):
        rows = pl.ds(pl.multiple_of(2 * block + shard * tokens, tokens), tokens)
        slot = jnp.where((way < 0) & (shard == me), heads, shard)
        return pltpu.make_async_remote_copy(
            src_ref=kv.at[g, :, rows, :],
            dst_ref=kv.at[g, :, rows, :],
            send_sem=z_send.at[slot, g],
            recv_sem=z_recv.at[shard, g],
            device_id={"head": lax.rem(me + way + heads, heads)},
            device_id_type=MESH,
        )

    def has_next(way):
        return (me + way >= 0) & (me + way < heads)

    def z_onward(g, shard, way):
        @pl.when(has_next(way))
        def _():
            z_copy(g, shard, way).start()

    def z_arrived(g, distance):
        for way in (1, -1):
            shard = me - way * distance

            @pl.when((shard >= 0) & (shard < heads))
            def _():
                z_copy(g, shard, way).wait_recv()
                z_onward(g, shard, way)
                pass_on(g, shard)

    def y_copy(g, shard):
        rows = pl.ds(pl.multiple_of(2 * block + shard * tokens, tokens), tokens)
        landing = pl.ds(pl.multiple_of(shard * tokens, tokens), tokens)
        return pltpu.make_async_remote_copy(
            src_ref=kv.at[g, :, rows, :],
            dst_ref=kv.at[g, :, landing, :],
            send_sem=y_send.at[shard, g],
            recv_sem=y_recv.at[shard, g],
            device_id=context(2),
            device_id_type=MESH,
        )

    def x_copy(g, shard):
        rows = pl.ds(pl.multiple_of((1 - odd) * 2 * block + shard * tokens, tokens), tokens)
        landing = pl.ds(pl.multiple_of(block + shard * tokens, tokens), tokens)
        return pltpu.make_async_remote_copy(
            src_ref=kv.at[g, :, rows, :],
            dst_ref=kv.at[g, :, landing, :],
            send_sem=x_send.at[shard, g],
            recv_sem=x_recv.at[shard, g],
            device_id=partner,
            device_id_type=MESH,
        )

    def y_needed(shard):
        return (odd == 1) | (shard >= me)

    def pass_on(g, shard):
        @pl.when(y_needed(shard))
        def _():
            y_copy(g, shard).start()

        @pl.when(odd == 0)
        def _():
            x_copy(g, shard).start()

    def y_arrived(g, shard):
        @pl.when(y_needed(shard))
        def _():
            y_copy(g, shard).wait_recv()

        @pl.when(odd == 1)
        def _():
            x_copy(g, shard).start()

    for g in range(groups):
        own_copy(g, 0).start()
        own_copy(g, 1).start()

    barrier = pltpu.get_barrier_semaphore()
    for distance in range(1, heads):
        pl.semaphore_signal(
            barrier, inc=1, device_id={"head": lax.rem(me + distance, heads)}, device_id_type=MESH
        )
    for place in (context(2), context(-2), partner):
        pl.semaphore_signal(barrier, inc=1, device_id=place, device_id_type=MESH)
    pl.semaphore_wait(barrier, heads - 1 + 3)

    for g in range(groups):
        own_copy(g, 0).wait()
        own_copy(g, 1).wait()
        z_onward(g, me, 1)
        z_onward(g, me, -1)
        pass_on(g, me)

    first = ctx * block + me * tokens
    query_pos = first + lax.broadcasted_iota(jnp.int32, (tokens, span), 0)
    key_pos = first - 2 * block + lax.broadcasted_iota(jnp.int32, (tokens, span), 1)
    row_pos = first + lax.broadcasted_iota(jnp.int32, (tokens, 128), 0)
    begin = jnp.zeros((tokens, 128), jnp.int32)
    end = jnp.int32(0)
    for n in range(lengths_ref.shape[0]):
        end = end + lengths_ref[n]
        begin = jnp.where(row_pos >= end, end, begin)
    visible = (key_pos >= begin[:, :1]) & (key_pos <= query_pos)
    bias[...] = jnp.where(visible, 0.0, -1e30)

    factor = math.log2(math.e) / math.sqrt(HEAD_SIZE)
    pair = 2 if width % 2 == 0 else 1
    reading = pl.ds(pl.multiple_of(me * tokens, tokens), span)

    def compute(g):
        key_part = kv.at[g, 0]
        value_part = kv.at[g, 1]

        def heads_of(j, carry):
            at = (g * width + j * pair) * HEAD_SIZE
            columns = [
                pl.ds(pl.multiple_of(at + p * HEAD_SIZE, HEAD_SIZE), HEAD_SIZE) for p in range(pair)
            ]
            q = jnp.concatenate([q_ref[:, c] for c in columns], axis=0)
            scores = lax.dot_general(
                q, key_part[reading, :], (((1,), (1,)), ((), ())), preferred_element_type=jnp.float32
            )
            scores = scores.reshape(pair, tokens, span) + bias[...][None]
            scores = scores.reshape(pair * tokens, span)
            top = jnp.max(scores, axis=1, keepdims=True)
            weights = jnp.exp2((scores - top) * factor)
            total = jnp.sum(weights, axis=1, keepdims=True)
            summed = jnp.dot(
                weights.astype(jnp.bfloat16), value_part[reading, :],
                preferred_element_type=jnp.float32,
            )
            result = (summed / total).astype(out_ref.dtype)
            for p in range(pair):
                out_ref[:, columns[p]] = result[p * tokens:(p + 1) * tokens]
            return carry

        lax.fori_loop(0, width // pair, heads_of, 0)

    def step(t, carry):
        for distance in range(1, heads):
            @pl.when((t >= distance - 1) & (t < groups + distance - 1))
            def _():
                z_arrived(t - distance + 1, distance)

        for distance in range(heads):
            @pl.when((t >= distance) & (t < groups + distance))
            def _():
                for shard in (me - distance, me + distance) if distance else (me,):
                    @pl.when((shard >= 0) & (shard < heads))
                    def _():
                        y_arrived(t - distance, shard)

        @pl.when(t >= heads)
        def _():
            for shard in range(heads):
                x_copy(t - heads, shard).wait_recv()
            compute(t - heads)

        return carry

    lax.fori_loop(0, groups + heads, step, 0)

    def drain(g, carry):
        for way in (1, -1):
            @pl.when(has_next(way))
            def _():
                z_copy(g, me, way).wait_send()

                for distance in range(1, heads):
                    shard = me - way * distance

                    @pl.when((shard >= 0) & (shard < heads))
                    def _():
                        z_copy(g, shard, way).wait_send()

        for shard in range(heads):
            @pl.when(y_needed(shard))
            def _():
                y_copy(g, shard).wait_send()

            x_copy(g, shard).wait_send()
        return carry

    lax.fori_loop(0, groups, drain, 0)


def solution(mesh):
    heads, outers, inners = (mesh.shape[name] for name in ("head", "outer", "inner"))

    def per_device(query, keys, values, lengths):
        tokens = query.shape[0]
        groups = keys.shape[1] // HEAD_SIZE
        return pl.pallas_call(
            functools.partial(kernel, heads, outers, inners),
            out_shape=jax.ShapeDtypeStruct(query.shape, query.dtype),
            in_specs=[
                pl.BlockSpec(memory_space=pltpu.SMEM),
                pl.BlockSpec(memory_space=pltpu.VMEM),
                pl.BlockSpec(memory_space=pl.ANY),
                pl.BlockSpec(memory_space=pl.ANY),
            ],
            out_specs=pl.BlockSpec(memory_space=pltpu.VMEM),
            scratch_shapes=[
                pltpu.VMEM((groups, 2, 3 * heads * tokens, HEAD_SIZE), jnp.bfloat16),
                pltpu.VMEM((tokens, (2 * heads + 1) * tokens), jnp.float32),
                pltpu.SemaphoreType.DMA((2, groups)),
                pltpu.SemaphoreType.DMA((heads + 1, groups)),
                pltpu.SemaphoreType.DMA((heads, groups)),
                pltpu.SemaphoreType.DMA((heads, groups)),
                pltpu.SemaphoreType.DMA((heads, groups)),
                pltpu.SemaphoreType.DMA((heads, groups)),
                pltpu.SemaphoreType.DMA((heads, groups)),
            ],
            compiler_params=pltpu.CompilerParams(collective_id=0, has_side_effects=True),
        )(lengths, query, keys, values)

    rows = P(("outer", "inner", "head"), None)
    return jax.shard_map(
        per_device,
        mesh=mesh,
        in_specs=(rows, rows, rows, P()),
        out_specs=rows,
        check_vma=False,
    )
```
